256 devices in a mesh: replica: 16 (over x, y_hi, core), tensor: 16 (over z, y_lo).
Axes of the slice: x: 4, y: 4 (y_hi: 2, y_lo: 2; y = y_hi * 2 + y_lo), z: 8, core: 2. Of those that a mesh axis runs over, the one named last changes fastest.
Arguments:
- inputs: bfloat16 [32768, 4096], P('replica', 'tensor'), may hold values from -6 to 6
- out_grad: bfloat16 [32768, 2560], P(('replica', 'tensor')), may hold values from -6 to 6
- weight: bfloat16 [4096, 2560], P('tensor'), may hold values from -0.09375 to 0.09375
- momentum: bfloat16 [16, 4096, 2560], P('replica', 'tensor'), may hold values from -6 to 6
- selected: int32 [2560, 64], P('tensor'), may hold values from 0 to 4095, as said below
Outputs:
- input_grad: bfloat16 [32768, 4096], P('replica', 'tensor')
- new_momentum: bfloat16 [16, 4096, 2560], P('replica', 'tensor')
- update: bfloat16 [4096, 2560], P('tensor')
The draws below stay inside these ranges and needn't reach their ends.
Inputs may be any that keep to these rules, and one draw needn't show every extreme that they name: `selected`: each row holds 64 different frequency numbers u * 64 + v of one block; the same selection holds for every replica.
All inputs are finite; a program needn't handle non-finite values.
Results may differ from the reference program's by a relative error of at most 0.001.
Values may be sent and summed in bfloat16 or wider, within the bound.
No kernel may reach another device: no remote copies, remote signals or barrier semaphores. Data moves between devices by JAX's collectives and lax.ppermute only.
A program may use at most 128 MiB of HBM per device.

```python
import math
import jax
import jax.numpy as jnp
from jax import lax

HQW = 4096
DW = 2560
BLK = 64
TOPK = 64
TOKR = 2048
TOKENS = 32768
NBLK = 2560
N_REPLICA = 16


def draw_selected(key, part):
    scores = jax.random.randint(key, (NBLK, BLK * BLK), 0, 2 ** 18) * (BLK * BLK) + jnp.arange(BLK * BLK, dtype=jnp.int32)[None, :]
    unused, chosen = lax.top_k(scores, TOPK)
    return chosen.astype(jnp.int32)


def block_levels(rng, extent, cuts, smallest, top_value):
    level = 1.0
    for axis_at, parts in cuts:
        steps = jax.random.uniform(jax.random.fold_in(jax.random.fold_in(rng, 6), axis_at), (parts,), jnp.float32, smallest / len(cuts), top_value / len(cuts))
        level = level * jnp.repeat(jnp.exp(steps), extent[axis_at] // parts).reshape((-1,) + (1,) * (len(extent) - 1 - axis_at))
    return level


def noise(own_key, dims, spread, limit, cuts=(), kind=jnp.bfloat16):
    result = jax.random.normal(own_key, dims, jnp.float32) * spread
    if len(cuts) > 0:
        result = block_levels(own_key, dims, cuts, -0.22, 0.18) * result
    return jnp.clip(result, min=-limit, max=limit).astype(kind)


def setup_inputs(seed: int = 0) -> dict:
    key_list = jax.random.split(jax.random.key(seed), 6)
    inputs = noise(key_list[0], (TOKENS, HQW), 1.0, 6.0, ((0, 16), (1, 16)))
    out_grad = noise(key_list[1], (TOKENS, DW), 1.0, 6.0, ((0, 256),))
    weight = noise(key_list[2], (HQW, DW), HQW ** -0.5, 0.09375, ((0, 16),))
    momentum = noise(key_list[3], (N_REPLICA, HQW, DW), 1.0, 6.0, ((0, 16), (1, 16)))
    selected = draw_selected(jax.random.fold_in(key_list[5], 71), 0)
    return dict(inputs=inputs, out_grad=out_grad, weight=weight, momentum=momentum, selected=selected)


HIGH = lax.Precision.HIGHEST

def basis_rows(freq):
    place = jnp.arange(BLK, dtype=jnp.float32)
    angle = math.pi * (2.0 * place + 1.0) / (2.0 * BLK)
    fvals = freq.astype(jnp.float32)[..., None]
    table = jnp.cos(fvals * angle) * math.sqrt(2.0 / BLK)
    return jnp.where(fvals == 0.0, math.sqrt(1.0 / BLK), table)

def bases(selected, rows, cols):
    row_basis = basis_rows(selected // BLK).reshape(rows // BLK, cols // BLK, TOPK, BLK)
    col_basis = basis_rows(selected % BLK).reshape(rows // BLK, cols // BLK, TOPK, BLK)
    return (row_basis, col_basis)

def encode_sel(matrix, row_basis, col_basis):
    grid = row_basis.shape
    split = matrix.reshape(grid[0], BLK, grid[1], BLK)
    proj = jnp.einsum('rcki,ricj->rckj', row_basis, split, precision=HIGH)
    return lax.optimization_barrier(jnp.sum(proj * col_basis, axis=-1)).reshape(grid[0] * grid[1], TOPK)

def decode_sel(values, row_basis, col_basis):
    grid = row_basis.shape
    weighted = col_basis * values.reshape(grid[0], grid[1], TOPK)[..., None]
    blocks = jnp.einsum('rcki,rckj->ricj', row_basis, weighted, precision=HIGH)
    return blocks.reshape(grid[0] * BLK, grid[1] * BLK)

def reference(inputs, out_grad, weight, momentum, selected):
    rows, cols = weight.shape
    row_basis, col_basis = bases(selected, rows, cols)
    scale = 1.0 / math.sqrt(TOKR)
    xs = inputs.reshape(N_REPLICA, TOKR, rows)
    gs = out_grad.reshape(N_REPLICA, TOKR, cols)

    def replica_step(items):
        acts, grads, moment = items
        wgrad = lax.dot_general(acts, grads, (((0,), (0,)), ((), ())), preferred_element_type=jnp.float32) * scale
        dacts = lax.dot_general(grads, weight, (((1,), (1,)), ((), ())), preferred_element_type=jnp.float32)
        accum = 0.999 * moment.astype(jnp.float32) + wgrad
        picked = encode_sel(accum, row_basis, col_basis)
        fresh = accum - decode_sel(picked, row_basis, col_basis)
        return (dacts.astype(jnp.bfloat16), fresh.astype(jnp.bfloat16), picked)
    dacts, fresh, picked = lax.map(replica_step, (xs, gs, momentum))
    mean_sent = lax.optimization_barrier(jnp.mean(picked, axis=0))
    update = BLK / math.sqrt(TOPK) * decode_sel(mean_sent, row_basis, col_basis)
    return (dacts.reshape(TOKENS, rows), fresh, update.astype(jnp.bfloat16))
```

```python
import math

import jax
import jax.numpy as jnp
import numpy as np
from jax import lax
from jax.experimental import pallas as pl
from jax.experimental.pallas import tpu as pltpu
from jax.sharding import Mesh
from jax.sharding import PartitionSpec as P


BLK = 64
TOPK = 64
TENSOR = ("z", "yl")
REPLICA = ("x", "yh", "core")

A1 = (0, 640)
A2 = (640, 1152)
B = (1152, 2560)
BCUT = 640
OFFSETS = (0, 1, -1, 2, -2, 3, -3, 4)


def dct_table():
    k = np.arange(BLK)
    table = np.cos(np.pi * np.outer(k, 2 * k + 1) / (2 * BLK)) * math.sqrt(2.0 / BLK)
    table[0] = math.sqrt(1.0 / BLK)
    return table.astype(np.float32)


def bf16_parts(table, n):
    parts, rest = [], table.astype(np.float32)
    for _ in range(n):
        part = rest.astype(jnp.bfloat16)
        parts.append(part)
        rest = rest - part.astype(np.float32)
    return parts


def dot(a, b, dims=((1,), (0,))):
    return lax.dot_general(a, b, (dims, ((), ())), preferred_element_type=jnp.float32)


def split(x):
    hi = x.astype(jnp.bfloat16)
    lo = (x - hi.astype(jnp.float32)).astype(jnp.bfloat16)
    return hi, lo


def vmem(n):
    return [pl.BlockSpec(memory_space=pltpu.VMEM)] * n


SMEM = pl.BlockSpec(memory_space=pltpu.SMEM)


def call(kernel, out, ins, specs):
    many = isinstance(out, (list, tuple))
    return pl.pallas_call(
        kernel,
        out_shape=out,
        in_specs=specs,
        out_specs=vmem(len(out)) if many else vmem(1)[0],
        cost_estimate=pl.CostEstimate(flops=10**9, bytes_accessed=0, transcendentals=0),
        compiler_params=pltpu.CompilerParams(vmem_limit_bytes=8 * 2**20),
    )(*ins)


def shape(s, d):
    return jax.ShapeDtypeStruct(s, d)


def prep_operands(idx, inputs, weight):
    tokens, rows = inputs.shape
    cols = weight.shape[1]

    def kernel(idx_ref, x_ref, w_ref, xt_ref, wt_ref):
        for s in range(tokens // 128):
            at = pl.multiple_of(idx_ref[s] * 128, 128)
            xt_ref[:, s * 128:(s + 1) * 128] = x_ref[pl.ds(at, 128), :].T
        for c in range(cols // 256):
            wt_ref[c * 256:(c + 1) * 256, :] = w_ref[:, c * 256:(c + 1) * 256].T

    return call(
        kernel,
        [shape((rows, tokens), jnp.bfloat16), shape((cols, rows), jnp.bfloat16)],
        (idx, inputs, weight),
        [SMEM] + vmem(2),
    )


def prep_bases(pairs):
    n = pairs.shape[0]
    table = dct_table()
    eye = np.eye(2, dtype=np.float32)

    def two(t):
        return [np.kron(eye, p.astype(np.float32)).astype(jnp.bfloat16) for p in bf16_parts(t, 2)]

    tt = jnp.asarray(np.concatenate(bf16_parts(table.T, 3), axis=1))
    t2 = jnp.asarray(np.concatenate(two(table.T), axis=0))
    g2 = jnp.asarray(np.concatenate(two(table), axis=1))

    def kernel(sel_ref, tt_ref, t2_ref, g2_ref, rt, ct, cd):
        lane = lax.broadcasted_iota(jnp.int32, (1, 128), 1)
        base = jnp.where(lane >= BLK, BLK, 0)
        row64 = lax.broadcasted_iota(jnp.int32, (BLK, 128), 0)
        row128 = lax.broadcasted_iota(jnp.int32, (128, 128), 0)
        for p in range(n):
            sel = sel_ref[p:p + 1, :]
            u = sel >> 6
            v = (sel & 63) + base
            ohu = jnp.where(row64 == u, 1.0, 0.0).astype(jnp.bfloat16)
            ohv = jnp.where(row128 == v, 1.0, 0.0).astype(jnp.bfloat16)
            rt[p] = dot(tt_ref[...], jnp.concatenate([ohu, ohu, ohu], axis=0))
            both = dot(t2_ref[...], ohv).astype(jnp.bfloat16)
            ct[p, :, :128] = both[:128]
            ct[p, :, 128:] = both[128:]
            cd[p] = dot(ohv, g2_ref[...], ((0,), (0,))).astype(jnp.bfloat16)

    return call(
        kernel,
        [shape((n, BLK, 128), jnp.float32), shape((n, 128, 256), jnp.bfloat16), shape((n, 128, 256), jnp.bfloat16)],
        (pairs, tt, t2, g2),
        vmem(4),
    )


def product(x, pair):
    n = x.shape[0]
    y = dot(jnp.concatenate(split(x), axis=0), pair)
    return (y[:n, :128] + y[n:, :128]) + (y[:n, 128:] + y[n:, 128:])


def wgrad_into(acc_ref, start, xt_ref, pieces, refs, scale):
    spans = sorted({(c, n) for _, _, c, n in pieces})
    edges = sorted({c for c, _ in spans} | {c + n for c, n in spans})
    for lo, hi in zip(edges[:-1], edges[1:]):
        for at in range(lo, hi, 256):
            width = min(256, hi - at)
            total = None
            for (slot, slots, c, n), ref in zip(pieces, refs):
                if not (c <= at and at + width <= c + n):
                    continue
                g = ref[..., at - c:at - c + width].reshape(slots * 128, width)
                part = dot(xt_ref[:, slot * 128:(slot + slots) * 128], g)
                total = part if total is None else total + part
            acc_ref[:, at:at + width] = start(at, width) + total * scale


def wgrad_first(xt, momentum, pieces, arrays, scale):
    rows, cols = momentum.shape

    def kernel(xt_ref, m_ref, *refs):
        acc_ref = refs[-1]
        wgrad_into(
            acc_ref,
            lambda at, n: 0.999 * m_ref[:, at:at + n].astype(jnp.float32),
            xt_ref, pieces, refs[:-1], scale,
        )

    return call(kernel, shape((rows, cols), jnp.float32), (xt, momentum, *arrays), vmem(2 + len(arrays)))


def wgrad_more(xt, acc, pieces, arrays, scale):
    def kernel(xt_ref, in_ref, *refs):
        wgrad_into(refs[-1], lambda at, n: in_ref[:, at:at + n], xt_ref, pieces, refs[:-1], scale)

    return call(kernel, shape(acc.shape, jnp.float32), (xt, acc, *arrays), vmem(2 + len(arrays)))


def wgrad_encode(xt, acc, pieces, arrays, rts, cts, scale):
    rows, cols = acc.shape
    brows = rows // BLK
    pcols = cols // 128

    def kernel(xt_ref, in_ref, *refs):
        rt, ct = refs[:brows], refs[brows:2 * brows]
        *ins, acc_ref, sent_ref = refs[2 * brows:]
        wgrad_into(acc_ref, lambda at, n: in_ref[:, at:at + n], xt_ref, pieces, ins, scale)
        for cp in range(pcols):
            for r in range(brows):
                p = r * pcols + cp
                u = product(acc_ref[r * BLK:(r + 1) * BLK, cp * 128:(cp + 1) * 128], ct[r][cp])
                sent_ref[p:p + 1, :] = jnp.sum(u * rt[r][cp], axis=0, keepdims=True)

    return call(
        kernel,
        [shape(acc.shape, jnp.float32), shape((brows * pcols, 128), jnp.float32)],
        (xt, acc, *rts, *cts, *arrays),
        vmem(2 + 2 * brows + len(arrays)),
    )


def residual(acc, sent, rts, cds):
    rows, cols = acc.shape
    pcols = cols // 128
    brows = rows // BLK

    def kernel(acc_ref, sent_ref, *refs):
        rt, cd, out_ref = refs[:brows], refs[brows:2 * brows], refs[-1]
        for cp in range(pcols):
            for r in range(brows):
                p = r * pcols + cp
                at = (slice(r * BLK, (r + 1) * BLK), slice(cp * 128, (cp + 1) * 128))
                e = product(rt[r][cp] * sent_ref[p:p + 1, :], cd[r][cp])
                out_ref[at] = (acc_ref[at] - e).astype(jnp.bfloat16)

    return call(kernel, shape(acc.shape, jnp.bfloat16), (acc, sent, *rts, *cds), vmem(2 + 2 * brows))


def decode_update(total, rts, cds, rows, cols, factor):
    pcols = cols // 128
    brows = rows // BLK

    def kernel(s_ref, *refs):
        rt, cd, out_ref = refs[:brows], refs[brows:2 * brows], refs[-1]
        for cp in range(pcols):
            for r in range(brows):
                p = r * pcols + cp
                at = (slice(r * BLK, (r + 1) * BLK), slice(cp * 128, (cp + 1) * 128))
                e = product(rt[r][cp] * (s_ref[p:p + 1, :] * factor), cd[r][cp])
                out_ref[at] = e.astype(jnp.bfloat16)

    return call(kernel, shape((rows, cols), jnp.bfloat16), (total, *rts, *cds), vmem(1 + 2 * brows))


def input_grad(idx, wt, slots, arrays, tokens, before):
    rows = wt.shape[1]
    given = [] if before is None else [before]

    def kernel(idx_ref, wt_ref, *refs):
        out_ref = refs[-1]
        if given:
            out_ref[...] = refs[-2][...]
        for s, pieces in slots:
            for dy in range(2):
                total = None
                for which, own, c, n in pieces:
                    if own is None:
                        g = refs[which][dy]
                    elif own == dy:
                        g = refs[which][...]
                    else:
                        continue
                    part = dot(g, wt_ref[c:c + n, :])
                    total = part if total is None else total + part
                at = pl.multiple_of(idx_ref[2 * s + dy] * 128, 128)
                out_ref[pl.ds(at, 128), :] = total.astype(jnp.bfloat16)

    return call(
        kernel,
        shape((tokens, rows), jnp.bfloat16),
        (idx, wt, *arrays, *given),
        [SMEM] + vmem(1 + len(arrays) + len(given)),
    )


def zp(x, step):
    n = lax.axis_size("z")
    return lax.ppermute(x, "z", [(i, (i + step) % n) for i in range(n)])


def yp(x):
    return lax.ppermute(x, "yl", [(0, 1), (1, 0)])


def over_replicas(s):
    def shift(v, axis, step):
        n = lax.axis_size(axis)
        return lax.ppermute(v, axis, [(i, (i + step) % n) for i in range(n)])

    a = shift(s, "yh", 1)
    b = lax.ppermute(s, ("yh", "core"), [(i, i ^ 3) for i in range(4)])
    c = shift(s, "core", 1)
    s = (s + c) + (a + b)
    e = shift(s, "x", 2)
    f = shift(s, "x", 1)
    g = shift(s, "x", -1)
    return (s + e) + (f + g)


def step(inputs, out_grad, weight, momentum, selected):
    rows, cols = weight.shape
    scale = 1.0 / math.sqrt(inputs.shape[0])
    z, yl = lax.axis_index("z"), lax.axis_index("yl")
    nz = lax.axis_size("z")
    idx = jnp.stack([((z - d) % nz) * 2 + (yl + dy) % 2 for d in OFFSETS for dy in range(2)]).astype(jnp.int32)

    a1, a2, b0 = (out_grad[:, lo:hi] for lo, hi in (A1, A2, B))

    xt, wt = prep_operands(idx, inputs, weight)
    pairs = selected.reshape(-1, 128)
    brows = rows // BLK
    per = pairs.shape[0] // brows
    rts, cts, cds = zip(*(prep_bases(pairs[per * r:per * (r + 1)]) for r in range(brows)))

    a1 = jnp.stack([a1, yp(a1)])
    a2 = jnp.stack([a2, yp(a2)])
    bz, ra1, ra2 = {0: b0}, {0: a1}, {0: a2}
    by = {0: yp(b0)}

    def ring(x, store, last):
        up = dn = x
        for d in (1, 2, 3):
            up, dn = zp(up, 1), zp(dn, -1)
            store[d], store[-d] = up, dn
        if last == "u":
            store[4] = zp(up, 1)
        elif last == "d":
            store[4] = zp(dn, -1)
        else:
            store[4] = zp(up[:, :BCUT], 1), zp(dn[:, BCUT:], -1)

    ring(b0, bz, None)
    ring(a1, ra1, "u")
    ring(a2, ra2, "d")
    for d in OFFSETS[1:-1]:
        by[d] = yp(bz[d])
    by[4] = tuple(yp(v) for v in bz[4])

    def entries(kind, d):
        slot = 2 * OFFSETS.index(d)
        if kind == "a1":
            return [((slot, 2, A1[0], A1[1] - A1[0]), ra1[d])]
        if kind == "a2":
            return [((slot, 2, A2[0], A2[1] - A2[0]), ra2[d])]
        slot, store = (slot, bz) if kind == "bz" else (slot + 1, by)
        if d == 4:
            return [
                ((slot, 1, B[0], BCUT), store[4][0]),
                ((slot, 1, B[0] + BCUT, B[1] - B[0] - BCUT), store[4][1]),
            ]
        return [((slot, 1, B[0], B[1] - B[0]), store[d])]

    stages = (
        [("bz", d) for d in (0, 1, -1, 2, -2, 3, -3)]
        + [("a1", d) for d in (0, 1, -1)] + [("a2", d) for d in (0, 1, -1)] + [("by", d) for d in (0, 1, -1)],
        [("bz", 4)] + [("by", d) for d in (2, -2, 3)] + [("a1", d) for d in (2, -2)] + [("a2", d) for d in (2, -2)],
        [("by", d) for d in (-3, 4)] + [("a1", d) for d in (3, -3, 4)] + [("a2", d) for d in (3, -3, 4)],
    )
    flat = []
    for stage in stages:
        es = [e for k, d in stage for e in entries(k, d)]
        flat.append(([e[0] for e in es], [e[1] for e in es]))

    acc = wgrad_first(xt, momentum[0], *flat[0], scale)
    acc = wgrad_more(xt, acc, *flat[1], scale)
    acc, sent = wgrad_encode(xt, acc, *flat[2], rts, cts, scale)
    total = over_replicas(sent)

    def input_part(offsets, before):
        arrays, slots = [], []

        def put(x):
            arrays.append(x)
            return len(arrays) - 1

        for d in offsets:
            these = [
                (put(ra1[d]), None, A1[0], A1[1] - A1[0]),
                (put(ra2[d]), None, A2[0], A2[1] - A2[0]),
            ]
            for own, store in enumerate((bz, by)):
                if d == 4:
                    these.append((put(store[4][0]), own, B[0], BCUT))
                    these.append((put(store[4][1]), own, B[0] + BCUT, B[1] - B[0] - BCUT))
                else:
                    these.append((put(store[d]), own, B[0], B[1] - B[0]))
            slots.append((OFFSETS.index(d), these))
        return input_grad(idx, wt, slots, arrays, inputs.shape[0], before)

    dacts = input_part((0, 1, -1), None)
    dacts = input_part((2, -2, 3, -3, 4), dacts)
    fresh = residual(acc, sent, rts, cds)
    factor = BLK / math.sqrt(TOPK) / math.prod(lax.axis_size(a) for a in REPLICA)
    update = decode_update(total, rts, cds, rows, cols, factor)
    return dacts, fresh[None], update


def solution(mesh):
    finer = Mesh(mesh.devices.reshape(4, 2, 2, 8, 2), REPLICA + TENSOR)
    whole = REPLICA + TENSOR
    in_specs = (P(REPLICA, TENSOR), P(whole, None), P(TENSOR, None), P(REPLICA, TENSOR, None), P(TENSOR, None))
    out_specs = (P(REPLICA, TENSOR), P(REPLICA, TENSOR, None), P(TENSOR, None))
    return jax.shard_map(step, mesh=finer, in_specs=in_specs, out_specs=out_specs, check_vma=False)
```

```python
import math

import jax
import jax.numpy as jnp
import numpy as np
from jax import lax
from jax.experimental import pallas as pl
from jax.experimental.pallas import tpu as pltpu
from jax.sharding import Mesh
from jax.sharding import PartitionSpec as P


BLK = 64
TOPK = 64
TENSOR = ("z", "yl")
REPLICA = ("x", "yh", "core")

CUT = 1152
A4 = 640
B4 = 640
OFFSETS = (0, 1, -1, 2, -2, 3, -3, 4)


def dct_table():
    k = np.arange(BLK)
    table = np.cos(np.pi * np.outer(k, 2 * k + 1) / (2 * BLK)) * math.sqrt(2.0 / BLK)
    table[0] = math.sqrt(1.0 / BLK)
    return table.astype(np.float32)


def bf16_parts(table, n):
    parts, rest = [], table.astype(np.float32)
    for _ in range(n):
        part = rest.astype(jnp.bfloat16)
        parts.append(part)
        rest = rest - part.astype(np.float32)
    return parts


def dot(a, b, dims=((1,), (0,))):
    return lax.dot_general(a, b, (dims, ((), ())), preferred_element_type=jnp.float32)


def split(x):
    hi = x.astype(jnp.bfloat16)
    lo = (x - hi.astype(jnp.float32)).astype(jnp.bfloat16)
    return hi, lo


def vmem(n):
    return [pl.BlockSpec(memory_space=pltpu.VMEM)] * n


SMEM = pl.BlockSpec(memory_space=pltpu.SMEM)


def call(kernel, out, ins, specs):
    many = isinstance(out, (list, tuple))
    return pl.pallas_call(
        kernel,
        out_shape=out,
        in_specs=specs,
        out_specs=vmem(len(out)) if many else vmem(1)[0],
        cost_estimate=pl.CostEstimate(flops=10**9, bytes_accessed=0, transcendentals=0),
        compiler_params=pltpu.CompilerParams(vmem_limit_bytes=8 * 2**20),
    )(*ins)


def shape(s, d):
    return jax.ShapeDtypeStruct(s, d)


def prep_operands(idx, inputs, weight):
    tokens, rows = inputs.shape
    cols = weight.shape[1]

    def kernel(idx_ref, x_ref, w_ref, xt_ref, wt_ref):
        for s in range(tokens // 128):
            at = pl.multiple_of(idx_ref[s] * 128, 128)
            xt_ref[:, s * 128:(s + 1) * 128] = x_ref[pl.ds(at, 128), :].T
        for c in range(cols // 256):
            wt_ref[c * 256:(c + 1) * 256, :] = w_ref[:, c * 256:(c + 1) * 256].T

    return call(
        kernel,
        [shape((rows, tokens), jnp.bfloat16), shape((cols, rows), jnp.bfloat16)],
        (idx, inputs, weight),
        [SMEM] + vmem(2),
    )


def prep_bases(selected, brows):
    blocks = selected.shape[0]
    per = blocks // 2 // brows
    table = dct_table()
    eye = np.eye(2, dtype=np.float32)
    tt = jnp.asarray(np.concatenate(bf16_parts(table.T, 3), axis=1))
    t2 = jnp.asarray(np.concatenate(bf16_parts(table.T, 2), axis=0))
    g2 = jnp.asarray(
        np.concatenate([np.kron(eye, p.astype(np.float32)).astype(jnp.bfloat16) for p in bf16_parts(table, 2)], axis=1)
    )

    def kernel(sel_ref, tt_ref, t2_ref, g2_ref, *outs):
        lane = lax.broadcasted_iota(jnp.int32, (1, 128), 1)
        base = jnp.where(lane >= BLK, BLK, 0)
        row64 = lax.broadcasted_iota(jnp.int32, (BLK, 128), 0)
        row128 = lax.broadcasted_iota(jnp.int32, (128, 128), 0)

        def one(r, cp):
            rt, ct, cd = outs[r], outs[brows + r], outs[2 * brows + r]
            at = (r * per + cp) * 2
            sel = jnp.concatenate([sel_ref[pl.ds(at, 1), :], sel_ref[pl.ds(at + 1, 1), :]], axis=1)
            u = sel >> 6
            v = sel & 63
            ohu = jnp.where(row64 == u, 1.0, 0.0).astype(jnp.bfloat16)
            ohv = jnp.where(row64 == v, 1.0, 0.0).astype(jnp.bfloat16)
            wide = jnp.where(row128 == v + base, 1.0, 0.0).astype(jnp.bfloat16)
            rt[cp] = dot(tt_ref[...], jnp.concatenate([ohu, ohu, ohu], axis=0))
            both = dot(t2_ref[...], ohv).astype(jnp.bfloat16)
            ct[cp, :, :128] = both[:BLK]
            ct[cp, :, 128:] = both[BLK:]
            full = dot(wide, g2_ref[...], ((0,), (0,)))
            cd[cp] = (full[:BLK] + full[BLK:]).astype(jnp.bfloat16)

        def group(g, _):
            for i in range(5):
                for r in range(brows):
                    one(r, g * 5 + i)
            return 0

        lax.fori_loop(0, per // 5, group, 0)

    f32 = [shape((per, BLK, 128), jnp.float32)] * brows
    b16 = [shape((per, BLK, 256), jnp.bfloat16)] * brows
    outs = call(kernel, f32 + b16 + b16, (selected, tt, t2, g2), vmem(4))
    return outs[:brows], outs[brows:2 * brows], outs[2 * brows:]


def product(x, pair):
    n = x.shape[0]
    lane = lax.broadcasted_iota(jnp.int32, (BLK, 256), 1)
    first = (lane & BLK) == 0
    none = jnp.zeros_like(pair)
    full = jnp.concatenate([jnp.where(first, pair, none), jnp.where(first, none, pair)], axis=0)
    y = dot(jnp.concatenate(split(x), axis=0), full)
    return (y[:n, :128] + y[n:, :128]) + (y[:n, 128:] + y[n:, 128:])


def over_pairs(brows, pcols, run):
    def group(g, _):
        for i in range(5):
            cp = g * 5 + i
            at = pl.ds(pl.multiple_of(cp * 128, 128), 128)
            for r in range(brows):
                run(r, cp, r * pcols + cp, slice(r * BLK, (r + 1) * BLK), at)
        return 0

    lax.fori_loop(0, pcols // 5, group, 0)


def distinct(pieces):
    arrays = list({id(p[0]): p[0] for p in pieces}.values())
    where = {id(x): i for i, x in enumerate(arrays)}
    return arrays, [(where[id(p[0])], *p[1:]) for p in pieces]


def view(refs, which, sub):
    return refs[which][...] if sub is None else refs[which][sub]


def wgrad_into(acc_ref, start, xt_ref, pieces, refs, scale):
    edges = sorted({p[4] for p in pieces} | {p[4] + p[5] for p in pieces} | {0, acc_ref.shape[1]})
    for lo, hi in zip(edges[:-1], edges[1:]):
        for at in range(lo, hi, 256):
            width = min(256, hi - at)
            total = None
            for which, sub, slot, slots, c, n in pieces:
                if not (c <= at and at + width <= c + n):
                    continue
                cut = slice(at - c, at - c + width)
                g = refs[which][..., cut] if sub is None else refs[which][sub, :, cut]
                part = dot(xt_ref[:, slot * 128:(slot + slots) * 128], g.reshape(slots * 128, width))
                total = part if total is None else total + part
            first = start(at, width)
            acc_ref[:, at:at + width] = first if total is None else first + total * scale


def wgrad_first(xt, momentum, pieces, scale):
    rows, cols = momentum.shape
    arrays, pieces = distinct(pieces)

    def kernel(xt_ref, m_ref, *refs):
        wgrad_into(
            refs[-1],
            lambda at, n: 0.999 * m_ref[:, at:at + n].astype(jnp.float32),
            xt_ref, pieces, refs[:-1], scale,
        )

    return call(kernel, shape((rows, cols), jnp.float32), (xt, momentum, *arrays), vmem(2 + len(arrays)))


def wgrad_more(xt, acc, pieces, scale):
    arrays, pieces = distinct(pieces)

    def kernel(xt_ref, in_ref, *refs):
        wgrad_into(refs[-1], lambda at, n: in_ref[:, at:at + n], xt_ref, pieces, refs[:-1], scale)

    return call(kernel, shape(acc.shape, jnp.float32), (xt, acc, *arrays), vmem(2 + len(arrays)))


def split_columns(g):
    n, cols = g.shape

    def kernel(g_ref, a_ref, b_ref):
        a_ref[...] = g_ref[:, :CUT]
        b_ref[...] = g_ref[:, CUT:]

    outs = [shape((n, CUT), g.dtype), shape((n, cols - CUT), g.dtype)]
    return call(kernel, outs, (g,), vmem(1))


def stacked(a, b):
    def kernel(a_ref, b_ref, out_ref):
        out_ref[0] = a_ref[...]
        out_ref[1] = b_ref[...]

    return call(kernel, shape((2, *a.shape), a.dtype), (a, b), vmem(2))


def beside(a, b):
    m = a.shape[1]

    def kernel(a_ref, b_ref, out_ref):
        out_ref[:, :m] = a_ref[...]
        out_ref[:, m:] = b_ref[...]

    return call(kernel, shape((a.shape[0], m + b.shape[1]), a.dtype), (a, b), vmem(2))


def wgrad_encode(xt, acc, pieces, rts, cts, scale):
    arrays, pieces = distinct(pieces)
    rows, cols = acc.shape
    brows = rows // BLK
    pcols = cols // 128

    def kernel(xt_ref, in_ref, *refs):
        rt, ct = refs[:brows], refs[brows:2 * brows]
        *ins, acc_ref, sent_ref = refs[2 * brows:]
        wgrad_into(acc_ref, lambda at, n: in_ref[:, at:at + n], xt_ref, pieces, ins, scale)

        def one(r, cp, p, at, cols_at):
            u = product(acc_ref[at, cols_at], ct[r][cp])
            sent_ref[pl.ds(p, 1), :] = jnp.sum(u * rt[r][cp], axis=0, keepdims=True)

        over_pairs(brows, pcols, one)

    return call(
        kernel,
        [shape(acc.shape, jnp.float32), shape((brows * pcols, 128), jnp.float32)],
        (xt, acc, *rts, *cts, *arrays),
        vmem(2 + 2 * brows + len(arrays)),
    )


def residual(acc, sent, rts, cds):
    rows, cols = acc.shape
    pcols = cols // 128
    brows = rows // BLK

    def kernel(acc_ref, sent_ref, *refs):
        rt, cd, out_ref = refs[:brows], refs[brows:2 * brows], refs[-1]

        def one(r, cp, p, at, cols_at):
            e = product(rt[r][cp] * sent_ref[pl.ds(p, 1), :], cd[r][cp])
            out_ref[at, cols_at] = (acc_ref[at, cols_at] - e).astype(jnp.bfloat16)

        over_pairs(brows, pcols, one)

    return call(kernel, shape(acc.shape, jnp.bfloat16), (acc, sent, *rts, *cds), vmem(2 + 2 * brows))


def decode_update(total, rts, cds, rows, cols, factor):
    pcols = cols // 128
    brows = rows // BLK

    def kernel(s_ref, *refs):
        rt, cd, out_ref = refs[:brows], refs[brows:2 * brows], refs[-1]

        def one(r, cp, p, at, cols_at):
            e = product(rt[r][cp] * (s_ref[pl.ds(p, 1), :] * factor), cd[r][cp])
            out_ref[at, cols_at] = e.astype(jnp.bfloat16)

        over_pairs(brows, pcols, one)

    return call(kernel, shape((rows, cols), jnp.bfloat16), (total, *rts, *cds), vmem(1 + 2 * brows))


def input_grad(idx, wt, pieces, tokens, before):
    rows = wt.shape[1]
    given = [] if before is None else [before]
    arrays, pieces = distinct(pieces)

    def kernel(idx_ref, wt_ref, *refs):
        out_ref = refs[-1]
        if given:
            out_ref[...] = refs[-2][...]
        for s in sorted({p[2] for p in pieces}):
            total = None
            for which, sub, slot, c, n in pieces:
                if slot == s:
                    part = dot(view(refs, which, sub), wt_ref[c:c + n, :])
                    total = part if total is None else total + part
            at = pl.multiple_of(idx_ref[s] * 128, 128)
            out_ref[pl.ds(at, 128), :] = total.astype(jnp.bfloat16)

    return call(
        kernel,
        shape((tokens, rows), jnp.bfloat16),
        (idx, wt, *arrays, *given),
        [SMEM] + vmem(1 + len(arrays) + len(given)),
    )


def zp(x, step):
    n = lax.axis_size("z")
    return lax.ppermute(x, "z", [(i, (i + step) % n) for i in range(n)])


def yp(x):
    return lax.ppermute(x, "yl", [(0, 1), (1, 0)])


def over_replicas(s):
    def shift(v, axis, step):
        n = lax.axis_size(axis)
        return lax.ppermute(v, axis, [(i, (i + step) % n) for i in range(n)])

    a = shift(s, "yh", 1)
    b = lax.ppermute(s, ("yh", "core"), [(i, i ^ 3) for i in range(4)])
    c = shift(s, "core", 1)
    s = (s + c) + (a + b)
    e = shift(s, "x", 2)
    f = shift(s, "x", 1)
    g = shift(s, "x", -1)
    return (s + e) + (f + g)


def step(inputs, out_grad, weight, momentum, selected):
    rows, cols = weight.shape
    scale = 1.0 / math.sqrt(inputs.shape[0])
    z, yl = lax.axis_index("z"), lax.axis_index("yl")
    nz = lax.axis_size("z")
    idx = jnp.stack([((z - d) % nz) * 2 + (yl + dy) % 2 for d in OFFSETS for dy in range(2)]).astype(jnp.int32)

    a, b = split_columns(out_grad)
    xt, wt = prep_operands(idx, inputs, weight)
    rts, cts, cds = prep_bases(selected, rows // BLK)

    def ring(x, cut):
        got = {0: x}
        up = dn = x
        for d in (1, 2, 3):
            up, dn = zp(up, 1), zp(dn, -1)
            got[d], got[-d] = up, dn
        got[4] = zp(up[..., :cut], 1), zp(dn[..., cut:], -1)
        return got

    ra = ring(stacked(a, yp(a)), A4)
    rb = ring(b, B4)
    own = {0: b, 4: beside(*rb[4])}
    own.update({d: stacked(rb[d], rb[-d]) for d in (1, 2, 3)})
    other = {d: yp(own[d]) for d in range(5)}

    def part_a(d):
        if d != 4:
            return [(ra[d], None, 0, CUT)]
        return [(ra[4][0], None, 0, A4), (ra[4][1], None, A4, CUT - A4)]

    def part_b(store, d):
        return store[abs(d)], (None if d in (0, 4) else int(d < 0)), CUT, cols - CUT

    def slot(d):
        return 2 * OFFSETS.index(d)

    def w_pieces(stage):
        pieces = []
        for kind, *offsets in stage:
            for d in offsets:
                if kind == "a":
                    pieces += [(x, sub, slot(d), 2, c, n) for x, sub, c, n in part_a(d)]
                else:
                    x, sub, c, n = part_b(own if kind == "own" else other, d)
                    pieces.append((x, sub, slot(d) + (kind == "other"), 1, c, n))
        return pieces

    acc = wgrad_first(xt, momentum[0], w_pieces([("own", 0, 1, -1), ("other", 0), ("a", 0, 1, -1)]), scale)
    acc = wgrad_more(xt, acc, w_pieces([("own", 2, -2, 3, -3), ("other", 1, -1, 2, -2), ("a", 2, -2)]), scale)
    acc = wgrad_more(xt, acc, w_pieces([("own", 4), ("a", 3, -3)]), scale)
    acc, sent = wgrad_encode(xt, acc, w_pieces([("other", 3, -3, 4), ("a", 4)]), rts, cts, scale)
    total = over_replicas(sent)

    def g_pieces(offsets):
        pieces = []
        for d in offsets:
            for dy, store in enumerate((own, other)):
                x, sub, c, n = part_b(store, d)
                pieces.append((x, sub, slot(d) + dy, c, n))
                pieces += [(x, dy, slot(d) + dy, c, n) for x, sub, c, n in part_a(d)]
        return pieces

    dacts = None
    for offsets in ((0, 1, -1), (2, -2), (3, -3), (4,)):
        dacts = input_grad(idx, wt, g_pieces(offsets), inputs.shape[0], dacts)
    fresh = residual(acc, sent, rts, cds)
    factor = BLK / math.sqrt(TOPK) / math.prod(lax.axis_size(a) for a in REPLICA)
    update = decode_update(total, rts, cds, rows, cols, factor)
    return dacts, fresh[None], update


def solution(mesh):
    finer = Mesh(mesh.devices.reshape(4, 2, 2, 8, 2), REPLICA + TENSOR)
    whole = REPLICA + TENSOR
    in_specs = (P(REPLICA, TENSOR), P(whole, None), P(TENSOR, None), P(REPLICA, TENSOR, None), P(TENSOR, None))
    out_specs = (P(REPLICA, TENSOR), P(REPLICA, TENSOR, None), P(TENSOR, None))
    return jax.shard_map(step, mesh=finer, in_specs=in_specs, out_specs=out_specs, check_vma=False)
```

```python
import math

import jax
import jax.numpy as jnp
import numpy as np
from jax import lax
from jax.experimental import pallas as pl
from jax.experimental.pallas import tpu as pltpu
from jax.sharding import Mesh
from jax.sharding import PartitionSpec as P


BLK = 64
TOPK = 64
TENSOR = ("z", "yl")
REPLICA = ("x", "yh", "core")

CUT = 1152
A4 = 640
B4 = 640
OFFSETS = (0, 1, -1, 2, -2, 3, -3, 4)


def dct_table():
    k = np.arange(BLK)
    table = np.cos(np.pi * np.outer(k, 2 * k + 1) / (2 * BLK)) * math.sqrt(2.0 / BLK)
    table[0] = math.sqrt(1.0 / BLK)
    return table.astype(np.float32)


def bf16_parts(table, n):
    parts, rest = [], table.astype(np.float32)
    for _ in range(n):
        part = rest.astype(jnp.bfloat16)
        parts.append(part)
        rest = rest - part.astype(np.float32)
    return parts


def dot(a, b, dims=((1,), (0,))):
    return lax.dot_general(a, b, (dims, ((), ())), preferred_element_type=jnp.float32)


def split(x):
    hi = x.astype(jnp.bfloat16)
    lo = (x - hi.astype(jnp.float32)).astype(jnp.bfloat16)
    return hi, lo


def vmem(n):
    return [pl.BlockSpec(memory_space=pltpu.VMEM)] * n


SMEM = pl.BlockSpec(memory_space=pltpu.SMEM)


def call(kernel, out, ins, specs):
    many = isinstance(out, (list, tuple))
    return pl.pallas_call(
        kernel,
        out_shape=out,
        in_specs=specs,
        out_specs=vmem(len(out)) if many else vmem(1)[0],
        cost_estimate=pl.CostEstimate(flops=10**9, bytes_accessed=0, transcendentals=0),
        compiler_params=pltpu.CompilerParams(vmem_limit_bytes=8 * 2**20),
    )(*ins)


def shape(s, d):
    return jax.ShapeDtypeStruct(s, d)


def prep_operands(idx, inputs, weight):
    tokens, rows = inputs.shape
    cols = weight.shape[1]

    def kernel(idx_ref, x_ref, w_ref, xt_ref, wt_ref):
        for s in range(tokens // 128):
            at = pl.multiple_of(idx_ref[s] * 128, 128)
            xt_ref[:, s * 128:(s + 1) * 128] = x_ref[pl.ds(at, 128), :].T
        for c in range(cols // 256):
            wt_ref[c * 256:(c + 1) * 256, :] = w_ref[:, c * 256:(c + 1) * 256].T

    return call(
        kernel,
        [shape((rows, tokens), jnp.bfloat16), shape((cols, rows), jnp.bfloat16)],
        (idx, inputs, weight),
        [SMEM] + vmem(2),
    )


def prep_bases(selected, brows):
    blocks = selected.shape[0]
    per = blocks // 2 // brows
    table = dct_table()
    eye = np.eye(2, dtype=np.float32)
    tt = jnp.asarray(np.concatenate(bf16_parts(table.T, 3), axis=1))
    t2 = jnp.asarray(np.concatenate(bf16_parts(table.T, 2), axis=0))
    g2 = jnp.asarray(
        np.concatenate([np.kron(eye, p.astype(np.float32)).astype(jnp.bfloat16) for p in bf16_parts(table, 2)], axis=1)
    )

    def kernel(sel_ref, tt_ref, t2_ref, g2_ref, *outs):
        lane = lax.broadcasted_iota(jnp.int32, (1, 128), 1)
        base = jnp.where(lane >= BLK, BLK, 0)
        row64 = lax.broadcasted_iota(jnp.int32, (BLK, 128), 0)
        row128 = lax.broadcasted_iota(jnp.int32, (128, 128), 0)

        def one(r, cp):
            rt, ct, cd = outs[r], outs[brows + r], outs[2 * brows + r]
            at = (r * per + cp) * 2
            sel = jnp.concatenate([sel_ref[pl.ds(at, 1), :], sel_ref[pl.ds(at + 1, 1), :]], axis=1)
            u = sel >> 6
            v = sel & 63
            ohu = jnp.where(row64 == u, 1.0, 0.0).astype(jnp.bfloat16)
            ohv = jnp.where(row64 == v, 1.0, 0.0).astype(jnp.bfloat16)
            wide = jnp.where(row128 == v + base, 1.0, 0.0).astype(jnp.bfloat16)
            rt[cp] = dot(tt_ref[...], jnp.concatenate([ohu, ohu, ohu], axis=0))
            both = dot(t2_ref[...], ohv).astype(jnp.bfloat16)
            ct[cp, :, :128] = both[:BLK]
            ct[cp, :, 128:] = both[BLK:]
            full = dot(wide, g2_ref[...], ((0,), (0,)))
            cd[cp] = (full[:BLK] + full[BLK:]).astype(jnp.bfloat16)

        def group(g, _):
            for i in range(5):
                for r in range(brows):
                    one(r, g * 5 + i)
            return 0

        lax.fori_loop(0, per // 5, group, 0)

    f32 = [shape((per, BLK, 128), jnp.float32)] * brows
    b16 = [shape((per, BLK, 256), jnp.bfloat16)] * brows
    outs = call(kernel, f32 + b16 + b16, (selected, tt, t2, g2), vmem(4))
    return outs[:brows], outs[brows:2 * brows], outs[2 * brows:]


def product(x, pair):
    n = x.shape[0]
    lane = lax.broadcasted_iota(jnp.int32, (BLK, 256), 1)
    first = (lane & BLK) == 0
    none = jnp.zeros_like(pair)
    full = jnp.concatenate([jnp.where(first, pair, none), jnp.where(first, none, pair)], axis=0)
    y = dot(jnp.concatenate(split(x), axis=0), full)
    return (y[:n, :128] + y[n:, :128]) + (y[:n, 128:] + y[n:, 128:])


def over_pairs(brows, first, last, run, at_once=None):
    cut = CUT // 128

    def number(r, cp):
        start, end = (0, cut) if first < cut else (cut, last)
        return start * brows + r * (end - start) + cp - start

    def some(cps):
        for cp in cps:
            at = cp * 128 if isinstance(cp, int) else pl.multiple_of(cp * 128, 128)
            for r in range(brows):
                run(r, cp, number(r, cp), slice(r * BLK, (r + 1) * BLK), pl.ds(at, 128))

    if at_once is None:
        some(range(first, last))
        return

    def group(g, _):
        some([first + g * at_once + i for i in range(at_once)])
        return 0

    whole = (last - first) // at_once
    lax.fori_loop(0, whole, group, 0)
    some(range(first + whole * at_once, last))


def distinct(pieces):
    arrays = list({id(p[0]): p[0] for p in pieces}.values())
    where = {id(x): i for i, x in enumerate(arrays)}
    return arrays, [(where[id(p[0])], *p[1:]) for p in pieces]


def view(refs, which, sub):
    return refs[which][...] if sub is None else refs[which][sub]


def wgrad_into(acc_ref, start, xt_ref, pieces, refs, scale):
    edges = sorted({p[4] for p in pieces} | {p[4] + p[5] for p in pieces} | {0, acc_ref.shape[1]})
    for lo, hi in zip(edges[:-1], edges[1:]):
        for at in range(lo, hi, 256):
            width = min(256, hi - at)
            total = None
            for which, sub, slot, slots, c, n in pieces:
                if not (c <= at and at + width <= c + n):
                    continue
                cut = slice(at - c, at - c + width)
                g = refs[which][..., cut] if sub is None else refs[which][sub, :, cut]
                part = dot(xt_ref[:, slot * 128:(slot + slots) * 128], g.reshape(slots * 128, width))
                total = part if total is None else total + part
            first = start(at, width)
            acc_ref[:, at:at + width] = first if total is None else first + total * scale


def wgrad_first(xt, momentum, pieces, scale):
    rows, cols = momentum.shape
    arrays, pieces = distinct(pieces)

    def kernel(xt_ref, m_ref, *refs):
        wgrad_into(
            refs[-1],
            lambda at, n: 0.999 * m_ref[:, at:at + n].astype(jnp.float32),
            xt_ref, pieces, refs[:-1], scale,
        )

    return call(kernel, shape((rows, cols), jnp.float32), (xt, momentum, *arrays), vmem(2 + len(arrays)))


def wgrad_more(xt, acc, pieces, scale):
    arrays, pieces = distinct(pieces)

    def kernel(xt_ref, in_ref, *refs):
        wgrad_into(refs[-1], lambda at, n: in_ref[:, at:at + n], xt_ref, pieces, refs[:-1], scale)

    return call(kernel, shape(acc.shape, jnp.float32), (xt, acc, *arrays), vmem(2 + len(arrays)))


def split_columns(g):
    n, cols = g.shape

    def kernel(g_ref, a_ref, b_ref):
        a_ref[...] = g_ref[:, :CUT]
        b_ref[...] = g_ref[:, CUT:]

    outs = [shape((n, CUT), g.dtype), shape((n, cols - CUT), g.dtype)]
    return call(kernel, outs, (g,), vmem(1))


def stacked(a, b):
    def kernel(a_ref, b_ref, out_ref):
        out_ref[0] = a_ref[...]
        out_ref[1] = b_ref[...]

    return call(kernel, shape((2, *a.shape), a.dtype), (a, b), vmem(2))


def beside(a, b):
    m = a.shape[1]

    def kernel(a_ref, b_ref, out_ref):
        out_ref[:, :m] = a_ref[...]
        out_ref[:, m:] = b_ref[...]

    return call(kernel, shape((a.shape[0], m + b.shape[1]), a.dtype), (a, b), vmem(2))


def wgrad_encode(xt, acc, pieces, rts, cts, scale, before):
    rows, cols = acc.shape
    brows = rows // BLK
    arrays, pieces = distinct(pieces)
    lo, hi = (0, CUT) if before is None else (CUT, cols)
    pieces = [(w, sub, slot, slots, c - lo, n) for w, sub, slot, slots, c, n in pieces]
    given = [] if before is None else [before]
    m = hi // 128 * brows

    def kernel(xt_ref, in_ref, *refs):
        rt, ct = refs[:brows], refs[brows:2 * brows]
        *ins, acc_ref, sent_ref = refs[2 * brows:]
        wgrad_into(acc_ref, lambda at, n: in_ref[:, lo + at:lo + at + n], xt_ref, pieces, ins, scale)
        if given:
            sent_ref[:lo // 128 * brows, :] = ins[-1][...]

        def one(r, cp, p, at, cols_at):
            u = product(acc_ref[at, cp * 128 - lo:cp * 128 - lo + 128], ct[r][cp])
            sent_ref[p:p + 1, :] = jnp.sum(u * rt[r][cp], axis=0, keepdims=True)

        over_pairs(brows, lo // 128, hi // 128, one)

    return call(
        kernel,
        [shape((rows, hi - lo), jnp.float32), shape((m, 128), jnp.float32)],
        (xt, acc, *rts, *cts, *arrays, *given),
        vmem(2 + 2 * brows + len(arrays) + len(given)),
    )


def residual(accs, sent, rts, cds):
    rows = accs[0].shape[0]
    cols = sum(x.shape[1] for x in accs)
    brows = rows // BLK

    def kernel(a_ref, b_ref, sent_ref, *refs):
        rt, cd, out_ref = refs[:brows], refs[brows:2 * brows], refs[-1]

        def walk(acc_ref, lo, hi):
            def one(r, cp, p, at, cols_at):
                e = product(rt[r][cp] * sent_ref[pl.ds(p, 1), :], cd[r][cp])
                here = pl.ds(pl.multiple_of(cp * 128 - lo, 128), 128)
                out_ref[at, cols_at] = (acc_ref[at, here] - e).astype(jnp.bfloat16)

            over_pairs(brows, lo // 128, hi // 128, one, 3)

        walk(a_ref, 0, CUT)
        walk(b_ref, CUT, cols)

    return call(kernel, shape((rows, cols), jnp.bfloat16), (*accs, sent, *rts, *cds), vmem(3 + 2 * brows))


def decode_update(total, rts, cds, rows, cols, factor):
    brows = rows // BLK

    def kernel(s_ref, *refs):
        rt, cd, out_ref = refs[:brows], refs[brows:2 * brows], refs[-1]

        def one(r, cp, p, at, cols_at):
            e = product(rt[r][cp] * (s_ref[p:p + 1, :] * factor), cd[r][cp])
            out_ref[at, cols_at] = e.astype(jnp.bfloat16)

        over_pairs(brows, 0, CUT // 128, one)
        over_pairs(brows, CUT // 128, cols // 128, one)

    return call(kernel, shape((rows, cols), jnp.bfloat16), (total, *rts, *cds), vmem(1 + 2 * brows))


def input_grad(idx, wt, pieces, tokens, before):
    rows = wt.shape[1]
    given = [] if before is None else [before]
    arrays, pieces = distinct(pieces)

    def kernel(idx_ref, wt_ref, *refs):
        out_ref = refs[-1]
        if given:
            out_ref[...] = refs[-2][...]
        for s in sorted({p[2] for p in pieces}):
            total = None
            for which, sub, slot, c, n in pieces:
                if slot == s:
                    part = dot(view(refs, which, sub), wt_ref[c:c + n, :])
                    total = part if total is None else total + part
            at = pl.multiple_of(idx_ref[s] * 128, 128)
            out_ref[pl.ds(at, 128), :] = total.astype(jnp.bfloat16)

    return call(
        kernel,
        shape((tokens, rows), jnp.bfloat16),
        (idx, wt, *arrays, *given),
        [SMEM] + vmem(1 + len(arrays) + len(given)),
    )


def zp(x, step):
    n = lax.axis_size("z")
    return lax.ppermute(x, "z", [(i, (i + step) % n) for i in range(n)])


def yp(x):
    return lax.ppermute(x, "yl", [(0, 1), (1, 0)])


def over_replicas(s):
    def shift(v, axis, step):
        n = lax.axis_size(axis)
        return lax.ppermute(v, axis, [(i, (i + step) % n) for i in range(n)])

    a = shift(s, "yh", 1)
    b = lax.ppermute(s, ("yh", "core"), [(i, i ^ 3) for i in range(4)])
    c = shift(s, "core", 1)
    s = (s + c) + (a + b)
    e = shift(s, "x", 2)
    f = shift(s, "x", 1)
    g = shift(s, "x", -1)
    return (s + e) + (f + g)


def step(inputs, out_grad, weight, momentum, selected):
    rows, cols = weight.shape
    scale = 1.0 / math.sqrt(inputs.shape[0])
    z, yl = lax.axis_index("z"), lax.axis_index("yl")
    nz = lax.axis_size("z")
    idx = jnp.stack([((z - d) % nz) * 2 + (yl + dy) % 2 for d in OFFSETS for dy in range(2)]).astype(jnp.int32)

    a, b = split_columns(out_grad)
    xt, wt = prep_operands(idx, inputs, weight)
    rts, cts, cds = prep_bases(selected, rows // BLK)

    def ring(x, cut):
        got = {0: x}
        up = dn = x
        for d in (1, 2, 3):
            up, dn = zp(up, 1), zp(dn, -1)
            got[d], got[-d] = up, dn
        got[4] = zp(up[..., :cut], 1), zp(dn[..., cut:], -1)
        return got

    ra = ring(stacked(a, yp(a)), A4)
    rb = ring(b, B4)
    own = {0: b, 4: beside(*rb[4])}
    own.update({d: stacked(rb[d], rb[-d]) for d in (1, 2, 3)})
    other = {d: yp(own[d]) for d in range(5)}

    def part_a(d):
        if d != 4:
            return [(ra[d], None, 0, CUT)]
        return [(ra[4][0], None, 0, A4), (ra[4][1], None, A4, CUT - A4)]

    def part_b(store, d):
        return store[abs(d)], (None if d in (0, 4) else int(d < 0)), CUT, cols - CUT

    def slot(d):
        return 2 * OFFSETS.index(d)

    def w_pieces(stage):
        pieces = []
        for kind, *offsets in stage:
            for d in offsets:
                if kind == "a":
                    pieces += [(x, sub, slot(d), 2, c, n) for x, sub, c, n in part_a(d)]
                else:
                    x, sub, c, n = part_b(own if kind == "own" else other, d)
                    pieces.append((x, sub, slot(d) + (kind == "other"), 1, c, n))
        return pieces

    acc = wgrad_first(xt, momentum[0], w_pieces([("own", 0, 1, -1), ("other", 0), ("a", 0, 1, -1)]), scale)
    acc = wgrad_more(xt, acc, w_pieces([("own", 2, -2, 3, -3), ("other", 1, -1, 2, -2), ("a", 2, -2)]), scale)
    acc = wgrad_more(xt, acc, w_pieces([("own", 4), ("a", 3, -3)]), scale)
    acc_a, sent_a = wgrad_encode(xt, acc, w_pieces([("a", 4)]), rts, cts, scale, None)
    acc_b, sent = wgrad_encode(xt, acc, w_pieces([("other", 3, -3, 4)]), rts, cts, scale, sent_a)
    total = over_replicas(sent)

    def g_pieces(offsets):
        pieces = []
        for d in offsets:
            for dy, store in enumerate((own, other)):
                x, sub, c, n = part_b(store, d)
                pieces.append((x, sub, slot(d) + dy, c, n))
                pieces += [(x, dy, slot(d) + dy, c, n) for x, sub, c, n in part_a(d)]
        return pieces

    dacts = None
    for offsets in ((0, 1, -1), (2, -2), (3, -3), (4,)):
        dacts = input_grad(idx, wt, g_pieces(offsets), inputs.shape[0], dacts)
    fresh = residual((acc_a, acc_b), sent, rts, cds)
    factor = BLK / math.sqrt(TOPK) / math.prod(lax.axis_size(a) for a in REPLICA)
    update = decode_update(total, rts, cds, rows, cols, factor)
    return dacts, fresh[None], update


def solution(mesh):
    finer = Mesh(mesh.devices.reshape(4, 2, 2, 8, 2), REPLICA + TENSOR)
    whole = REPLICA + TENSOR
    in_specs = (P(REPLICA, TENSOR), P(whole, None), P(TENSOR, None), P(REPLICA, TENSOR, None), P(TENSOR, None))
    out_specs = (P(REPLICA, TENSOR), P(REPLICA, TENSOR, None), P(TENSOR, None))
    return jax.shard_map(step, mesh=finer, in_specs=in_specs, out_specs=out_specs, check_vma=False)
```

```python
import math

import jax
import jax.numpy as jnp
import numpy as np
from jax import lax
from jax.experimental import pallas as pl
from jax.experimental.pallas import tpu as pltpu
from jax.sharding import Mesh
from jax.sharding import PartitionSpec as P


BLK = 64
TOPK = 64
TENSOR = ("z", "yl")
REPLICA = ("x", "yh", "core")

CUT = 1024
B4 = 768
OFFSETS = (0, 1, -1, 2, -2, 3, -3, 4)


def dct_table():
    k = np.arange(BLK)
    table = np.cos(np.pi * np.outer(k, 2 * k + 1) / (2 * BLK)) * math.sqrt(2.0 / BLK)
    table[0] = math.sqrt(1.0 / BLK)
    return table.astype(np.float32)


def bf16_parts(table, n):
    parts, rest = [], table.astype(np.float32)
    for _ in range(n):
        part = rest.astype(jnp.bfloat16)
        parts.append(part)
        rest = rest - part.astype(np.float32)
    return parts


def dot(a, b, dims=((1,), (0,))):
    return lax.dot_general(a, b, (dims, ((), ())), preferred_element_type=jnp.float32)


def split(x):
    hi = x.astype(jnp.bfloat16)
    lo = (x - hi.astype(jnp.float32)).astype(jnp.bfloat16)
    return hi, lo


def vmem(n):
    return [pl.BlockSpec(memory_space=pltpu.VMEM)] * n


SMEM = pl.BlockSpec(memory_space=pltpu.SMEM)


def call(kernel, out, ins, specs):
    many = isinstance(out, (list, tuple))
    return pl.pallas_call(
        kernel,
        out_shape=out,
        in_specs=specs,
        out_specs=vmem(len(out)) if many else vmem(1)[0],
        cost_estimate=pl.CostEstimate(flops=10**10, bytes_accessed=0, transcendentals=0),
        compiler_params=pltpu.CompilerParams(vmem_limit_bytes=8 * 2**20),
    )(*ins)


def shape(s, d):
    return jax.ShapeDtypeStruct(s, d)


def prep_operands(idx, inputs, weight):
    tokens, rows = inputs.shape
    cols = weight.shape[1]

    def kernel(idx_ref, x_ref, w_ref, xt_ref, wt_ref):
        for s in range(tokens // 128):
            at = pl.multiple_of(idx_ref[s] * 128, 128)
            xt_ref[:, s * 128:(s + 1) * 128] = x_ref[pl.ds(at, 128), :].T
        for c in range(cols // 256):
            wt_ref[c * 256:(c + 1) * 256, :] = w_ref[:, c * 256:(c + 1) * 256].T

    return call(
        kernel,
        [shape((rows, tokens), jnp.bfloat16), shape((cols, rows), jnp.bfloat16)],
        (idx, inputs, weight),
        [SMEM] + vmem(2),
    )


def prep_bases(selected, brows):
    blocks = selected.shape[0]
    per = blocks // 2 // brows
    table = dct_table()
    eye = np.eye(2, dtype=np.float32)
    tt = jnp.asarray(np.concatenate(bf16_parts(table.T, 3), axis=1))
    t2 = jnp.asarray(np.concatenate(bf16_parts(table.T, 2), axis=0))
    g2 = jnp.asarray(
        np.concatenate([np.kron(eye, p.astype(np.float32)).astype(jnp.bfloat16) for p in bf16_parts(table, 2)], axis=1)
    )

    def kernel(sel_ref, tt_ref, t2_ref, g2_ref, *outs):
        lane = lax.broadcasted_iota(jnp.int32, (1, 128), 1)
        base = jnp.where(lane >= BLK, BLK, 0)
        row64 = lax.broadcasted_iota(jnp.int32, (BLK, 128), 0)
        row128 = lax.broadcasted_iota(jnp.int32, (128, 128), 0)

        def one(r, cp):
            rt, ct, cd = outs[r], outs[brows + r], outs[2 * brows + r]
            at = (r * per + cp) * 2
            sel = jnp.concatenate([sel_ref[pl.ds(at, 1), :], sel_ref[pl.ds(at + 1, 1), :]], axis=1)
            u = sel >> 6
            v = sel & 63
            ohu = jnp.where(row64 == u, 1.0, 0.0).astype(jnp.bfloat16)
            ohv = jnp.where(row64 == v, 1.0, 0.0).astype(jnp.bfloat16)
            wide = jnp.where(row128 == v + base, 1.0, 0.0).astype(jnp.bfloat16)
            rt[cp] = dot(tt_ref[...], jnp.concatenate([ohu, ohu, ohu], axis=0))
            both = dot(t2_ref[...], ohv).astype(jnp.bfloat16)
            ct[cp, :, :128] = both[:BLK]
            ct[cp, :, 128:] = both[BLK:]
            full = dot(wide, g2_ref[...], ((0,), (0,)))
            cd[cp] = (full[:BLK] + full[BLK:]).astype(jnp.bfloat16)

        def group(g, _):
            for i in range(5):
                for r in range(brows):
                    one(r, g * 5 + i)
            return 0

        lax.fori_loop(0, per // 5, group, 0)

    f32 = [shape((per, BLK, 128), jnp.float32)] * brows
    b16 = [shape((per, BLK, 256), jnp.bfloat16)] * brows
    outs = call(kernel, f32 + b16 + b16, (selected, tt, t2, g2), vmem(4))
    return outs[:brows], outs[brows:2 * brows], outs[2 * brows:]


def product(x, pair):
    n = x.shape[0]
    lane = lax.broadcasted_iota(jnp.int32, (BLK, 256), 1)
    first = (lane & BLK) == 0
    none = jnp.zeros_like(pair)
    full = jnp.concatenate([jnp.where(first, pair, none), jnp.where(first, none, pair)], axis=0)
    y = dot(jnp.concatenate(split(x), axis=0), full)
    return (y[:n, :128] + y[n:, :128]) + (y[:n, 128:] + y[n:, 128:])


def over_pairs(brows, first, last, run, at_once=None):
    cut = CUT // 128

    def number(r, cp):
        start, end = (0, cut) if first < cut else (cut, last)
        return start * brows + r * (end - start) + cp - start

    def some(cps):
        for cp in cps:
            at = cp * 128 if isinstance(cp, int) else pl.multiple_of(cp * 128, 128)
            for r in range(brows):
                run(r, cp, number(r, cp), slice(r * BLK, (r + 1) * BLK), pl.ds(at, 128))

    if at_once is None:
        some(range(first, last))
        return

    def group(g, _):
        some([first + g * at_once + i for i in range(at_once)])
        return 0

    whole = (last - first) // at_once
    lax.fori_loop(0, whole, group, 0)
    some(range(first + whole * at_once, last))


def distinct(pieces):
    arrays = list({id(p[0]): p[0] for p in pieces}.values())
    where = {id(x): i for i, x in enumerate(arrays)}
    return arrays, [(where[id(p[0])], *p[1:]) for p in pieces]


def view(refs, which, sub):
    return refs[which][...] if sub is None else refs[which][sub]


def wgrad_into(acc_ref, start, xt_ref, pieces, refs, scale):
    edges = sorted({p[4] for p in pieces} | {p[4] + p[5] for p in pieces} | {0, acc_ref.shape[1]})
    for lo, hi in zip(edges[:-1], edges[1:]):
        for at in range(lo, hi, 256):
            width = min(256, hi - at)
            total = None
            for which, sub, slot, slots, c, n in pieces:
                if not (c <= at and at + width <= c + n):
                    continue
                cut = slice(at - c, at - c + width)
                g = refs[which][..., cut] if sub is None else refs[which][sub, :, cut]
                part = dot(xt_ref[:, slot * 128:(slot + slots) * 128], g.reshape(slots * 128, width))
                total = part if total is None else total + part
            first = start(at, width)
            acc_ref[:, at:at + width] = first if total is None else first + total * scale


def wgrad_first(xt, momentum, pieces, scale):
    rows, cols = momentum.shape
    arrays, pieces = distinct(pieces)

    def kernel(xt_ref, m_ref, *refs):
        wgrad_into(
            refs[-1],
            lambda at, n: 0.999 * m_ref[:, at:at + n].astype(jnp.float32),
            xt_ref, pieces, refs[:-1], scale,
        )

    return call(kernel, shape((rows, cols), jnp.float32), (xt, momentum, *arrays), vmem(2 + len(arrays)))


def wgrad_more(xt, acc, pieces, scale):
    arrays, pieces = distinct(pieces)

    def kernel(xt_ref, in_ref, *refs):
        wgrad_into(refs[-1], lambda at, n: in_ref[:, at:at + n], xt_ref, pieces, refs[:-1], scale)

    return call(kernel, shape(acc.shape, jnp.float32), (xt, acc, *arrays), vmem(2 + len(arrays)))


def split_columns(g):
    n, cols = g.shape

    def kernel(g_ref, a_ref, b_ref):
        a_ref[...] = g_ref[:, :CUT]
        b_ref[...] = g_ref[:, CUT:]

    outs = [shape((n, CUT), g.dtype), shape((n, cols - CUT), g.dtype)]
    return call(kernel, outs, (g,), vmem(1))


def stacked(a, b):
    def kernel(a_ref, b_ref, out_ref):
        out_ref[0] = a_ref[...]
        out_ref[1] = b_ref[...]

    return call(kernel, shape((2, *a.shape), a.dtype), (a, b), vmem(2))


def beside(a, b):
    m = a.shape[1]

    def kernel(a_ref, b_ref, out_ref):
        out_ref[:, :m] = a_ref[...]
        out_ref[:, m:] = b_ref[...]

    return call(kernel, shape((a.shape[0], m + b.shape[1]), a.dtype), (a, b), vmem(2))


def wgrad_encode(xt, acc, pieces, rts, cts, scale, before):
    rows, cols = acc.shape
    brows = rows // BLK
    arrays, pieces = distinct(pieces)
    lo, hi = (0, CUT) if before is None else (CUT, cols)
    pieces = [(w, sub, slot, slots, c - lo, n) for w, sub, slot, slots, c, n in pieces]
    given = [] if before is None else [before]
    m = hi // 128 * brows

    def kernel(xt_ref, in_ref, *refs):
        rt, ct = refs[:brows], refs[brows:2 * brows]
        *ins, acc_ref, sent_ref = refs[2 * brows:]
        wgrad_into(acc_ref, lambda at, n: in_ref[:, lo + at:lo + at + n], xt_ref, pieces, ins, scale)
        if given:
            sent_ref[:lo // 128 * brows, :] = ins[-1][...]

        def one(r, cp, p, at, cols_at):
            here = pl.ds(pl.multiple_of(cp * 128 - lo, 128), 128)
            u = product(acc_ref[at, here], ct[r][cp])
            sent_ref[pl.ds(p, 1), :] = jnp.sum(u * rt[r][cp], axis=0, keepdims=True)

        over_pairs(brows, lo // 128, hi // 128, one, 4)

    return call(
        kernel,
        [shape((rows, hi - lo), jnp.float32), shape((m, 128), jnp.float32)],
        (xt, acc, *rts, *cts, *arrays, *given),
        vmem(2 + 2 * brows + len(arrays) + len(given)),
    )


def residual(accs, sent, rts, cds):
    rows = accs[0].shape[0]
    cols = sum(x.shape[1] for x in accs)
    brows = rows // BLK

    def kernel(a_ref, b_ref, sent_ref, *refs):
        rt, cd, out_ref = refs[:brows], refs[brows:2 * brows], refs[-1]

        def walk(acc_ref, lo, hi):
            def one(r, cp, p, at, cols_at):
                e = product(rt[r][cp] * sent_ref[pl.ds(p, 1), :], cd[r][cp])
                here = pl.ds(pl.multiple_of(cp * 128 - lo, 128), 128)
                out_ref[at, cols_at] = (acc_ref[at, here] - e).astype(jnp.bfloat16)

            over_pairs(brows, lo // 128, hi // 128, one, 4)

        walk(a_ref, 0, CUT)
        walk(b_ref, CUT, cols)

    return call(kernel, shape((rows, cols), jnp.bfloat16), (*accs, sent, *rts, *cds), vmem(3 + 2 * brows))


def decode_update(total, rts, cds, rows, cols, factor):
    brows = rows // BLK

    def kernel(s_ref, *refs):
        rt, cd, out_ref = refs[:brows], refs[brows:2 * brows], refs[-1]

        def one(r, cp, p, at, cols_at):
            e = product(rt[r][cp] * (s_ref[p:p + 1, :] * factor), cd[r][cp])
            out_ref[at, cols_at] = e.astype(jnp.bfloat16)

        over_pairs(brows, 0, CUT // 128, one)
        over_pairs(brows, CUT // 128, cols // 128, one)

    return call(kernel, shape((rows, cols), jnp.bfloat16), (total, *rts, *cds), vmem(1 + 2 * brows))


def input_grad(idx, wt, pieces, tokens, before):
    rows = wt.shape[1]
    given = [] if before is None else [before]
    arrays, pieces = distinct(pieces)

    def kernel(idx_ref, wt_ref, *refs):
        out_ref = refs[-1]
        if given:
            out_ref[...] = refs[-2][...]
        for s in sorted({p[2] for p in pieces}):
            total = None
            for which, sub, slot, c, n in pieces:
                if slot == s:
                    part = dot(view(refs, which, sub), wt_ref[c:c + n, :])
                    total = part if total is None else total + part
            at = pl.multiple_of(idx_ref[s] * 128, 128)
            out_ref[pl.ds(at, 128), :] = total.astype(jnp.bfloat16)

    return call(
        kernel,
        shape((tokens, rows), jnp.bfloat16),
        (idx, wt, *arrays, *given),
        [SMEM] + vmem(1 + len(arrays) + len(given)),
    )


def zp(x, step):
    n = lax.axis_size("z")
    return lax.ppermute(x, "z", [(i, (i + step) % n) for i in range(n)])


def yp(x):
    return lax.ppermute(x, "yl", [(0, 1), (1, 0)])


def over_replicas(s):
    def shift(v, axis, step):
        n = lax.axis_size(axis)
        return lax.ppermute(v, axis, [(i, (i + step) % n) for i in range(n)])

    a = shift(s, "yh", 1)
    b = lax.ppermute(s, ("yh", "core"), [(i, i ^ 3) for i in range(4)])
    c = shift(s, "core", 1)
    s = (s + c) + (a + b)
    e = shift(s, "x", 2)
    f = shift(s, "x", 1)
    g = shift(s, "x", -1)
    return (s + e) + (f + g)


def step(inputs, out_grad, weight, momentum, selected):
    rows, cols = weight.shape
    scale = 1.0 / math.sqrt(inputs.shape[0])
    z, yl = lax.axis_index("z"), lax.axis_index("yl")
    nz = lax.axis_size("z")
    idx = jnp.stack([((z - d) % nz) * 2 + (yl + dy) % 2 for d in OFFSETS for dy in range(2)]).astype(jnp.int32)

    a, b = split_columns(out_grad)
    xt, wt = prep_operands(idx, inputs, weight)
    rts, cts, cds = prep_bases(selected, rows // BLK)

    def ring(x, cut):
        got = {0: x}
        up = dn = x
        for d in (1, 2, 3):
            up, dn = zp(up, 1), zp(dn, -1)
            got[d], got[-d] = up, dn
        if cut == "up":
            got[4] = zp(up, 1)
        elif cut == "down":
            got[4] = zp(dn, -1)
        else:
            got[4] = zp(up[:, :cut], 1), zp(dn[:, cut:], -1)
        return got

    ra = ring(a, "up"), ring(yp(a), "down")
    rb = ring(b, B4)
    own = {0: b, 4: beside(*rb[4])}
    own.update({d: stacked(rb[d], rb[-d]) for d in (1, 2, 3)})
    other = {d: yp(own[d]) for d in range(5)}

    def part_b(store, d):
        return store[abs(d)], (None if d in (0, 4) else int(d < 0)), CUT, cols - CUT

    def slot(d):
        return 2 * OFFSETS.index(d)

    def w_pieces(stage):
        pieces = []
        for kind, *offsets in stage:
            for d in offsets:
                if kind == "a":
                    pieces += [(ra[dy][d], None, slot(d) + dy, 1, 0, CUT) for dy in range(2)]
                else:
                    x, sub, c, n = part_b(own if kind == "own" else other, d)
                    pieces.append((x, sub, slot(d) + (kind == "other"), 1, c, n))
        return pieces

    acc = wgrad_first(xt, momentum[0], w_pieces([("own", 0, 1, -1), ("other", 0), ("a", 0, 1, -1)]), scale)
    acc = wgrad_more(xt, acc, w_pieces([("own", 2, -2, 3, -3), ("other", 1, -1, 2, -2), ("a", 2, -2)]), scale)
    acc = wgrad_more(xt, acc, w_pieces([("own", 4), ("other", 3, -3), ("a", 3, -3)]), scale)
    acc_a, sent_a = wgrad_encode(xt, acc, w_pieces([("a", 4)]), rts, cts, scale, None)
    acc_b, sent = wgrad_encode(xt, acc, w_pieces([("other", 4)]), rts, cts, scale, sent_a)
    total = over_replicas(sent)

    def g_pieces(offsets):
        pieces = []
        for d in offsets:
            for dy, store in enumerate((own, other)):
                x, sub, c, n = part_b(store, d)
                pieces.append((x, sub, slot(d) + dy, c, n))
                pieces.append((ra[dy][d], None, slot(d) + dy, 0, CUT))
        return pieces

    dacts = None
    for offsets in ((0, 1, -1), (2, -2), (3, -3), (4,)):
        dacts = input_grad(idx, wt, g_pieces(offsets), inputs.shape[0], dacts)
    fresh = residual((acc_a, acc_b), sent, rts, cds)
    factor = BLK / math.sqrt(TOPK) / math.prod(lax.axis_size(a) for a in REPLICA)
    update = decode_update(total, rts, cds, rows, cols, factor)
    return dacts, fresh[None], update


def solution(mesh):
    finer = Mesh(mesh.devices.reshape(4, 2, 2, 8, 2), REPLICA + TENSOR)
    whole = REPLICA + TENSOR
    in_specs = (P(REPLICA, TENSOR), P(whole, None), P(TENSOR, None), P(REPLICA, TENSOR, None), P(TENSOR, None))
    out_specs = (P(REPLICA, TENSOR), P(REPLICA, TENSOR, None), P(TENSOR, None))
    return jax.shard_map(step, mesh=finer, in_specs=in_specs, out_specs=out_specs, check_vma=False)
```
